32 devices in a mesh: grp: 4 (over y, core), sp: 8 (over z, x).
Axes of the slice: x: 2, y: 2, z: 4, core: 2. Of those that a mesh axis runs over, the one named last changes fastest.
Arguments:
- bucket_of: int32 [4], replicated, may hold values from 0 to 3, as said below
- lengths: int32 [4], replicated, may hold values from 128 to 512, as said below
- counts: int32 [4], replicated, may hold values from 256 to 4096
- queries: bfloat16 [4096, 4096], P(('grp', 'sp')), may hold values from -4.5 to 4.5
- keys: bfloat16 [4096, 4096], P(('grp', 'sp')), may hold values from -4.5 to 4.5
- values: bfloat16 [4096, 4096], P(('grp', 'sp')), may hold values from -6 to 6
- out_grad: bfloat16 [4096, 3072], P(('grp', 'sp')), may hold values from -6 to 6
- w_out: bfloat16 [4096, 3072], P('sp', 'grp'), may hold values from -1.75 to 1.75
Outputs:
- grad_queries: bfloat16 [4096, 4096], P(('grp', 'sp'))
- grad_keys: bfloat16 [4096, 4096], P(('grp', 'sp'))
- grad_values: bfloat16 [4096, 4096], P(('grp', 'sp'))
- grad_w_out: float32 [4096, 3072], P('sp', 'grp')
The draws below stay inside these ranges and needn't reach their ends.
Inputs may be any that keep to these rules, and one draw needn't show every extreme that they name: `bucket_of`: every one of the 4 buckets is held by at least one group. `lengths`: one bucket has length exactly 512.
All inputs are finite; a program needn't handle non-finite values.
Results may differ from the reference program's by a relative error of at most 0.0091.
Values may be sent and summed in bfloat16 or wider, within the bound.
A program may use at most 128 MiB of HBM per device.

```python
from functools import partial
import jax
import jax.numpy as jnp
from jax import lax

D = 3072
HEAD_DIM = 128
SEQS = 2
NB = 4
GROUPS = 4
GTOK = 1024
CAP = 512
HD = 4096
TOKENS = 4096


def shared_pattern(key):
    pattern_key = jax.random.fold_in(key, 404)
    signs = jnp.where(jax.random.bernoulli(jax.random.fold_in(pattern_key, 1), 0.5, (HD,)), 4.5, -4.5)
    query_spot = jax.random.randint(jax.random.fold_in(pattern_key, 2), (), 0, CAP)
    key_spot = jax.random.randint(jax.random.fold_in(pattern_key, 3), (), 0, max(CAP // 4, 1))
    return (signs, query_spot, key_spot)


def draw_queries(key, part):
    signs, query_spot, key_spot = shared_pattern(key)
    own_key = jax.random.fold_in(key, 11)
    filled = jnp.clip(jax.random.normal(own_key, (TOKENS, HD)), -4.5, 4.5)
    return filled.astype(jnp.bfloat16)


def draw_keys(key, part):
    signs, query_spot, key_spot = shared_pattern(key)
    own_key = jax.random.fold_in(key, 12)
    filled = jnp.clip(jax.random.normal(own_key, (TOKENS, HD)), -4.5, 4.5)
    return filled.astype(jnp.bfloat16)


def draw_bucket_of(key, part):
    first = jax.random.permutation(jax.random.fold_in(key, 21), NB).astype(jnp.int32)
    others = jax.random.randint(jax.random.fold_in(key, 22), (GROUPS,), 0, NB).astype(jnp.int32)
    listed = jnp.concatenate([first, others])[:GROUPS]
    return jax.random.permutation(jax.random.fold_in(key, 23), listed).astype(jnp.int32)


def draw_lengths(key, part):
    drawn = jax.random.randint(jax.random.fold_in(key, 31), (NB,), CAP // 4, CAP + 1)
    longest = jax.random.randint(jax.random.fold_in(key, 32), (), 0, NB)
    return jnp.where(jnp.arange(NB) == longest, CAP, drawn).astype(jnp.int32)


def touch_ends(array, stream_key, least, largest):
    extent = array.shape
    place = [jax.random.randint(jax.random.fold_in(stream_key, axis), (), 0, extent[axis]) for axis in range(len(extent))]
    array = array.at[tuple(place)].set(least)
    longest = extent.index(max(extent))
    place[longest] = (place[longest] + 1) % extent[longest]
    return array.at[tuple(place)].set(largest)


def spiked(array, stream_key, source, target, shards_of, factor):
    owner, partner = [(jnp.arange(array.shape[axis_at]) // (array.shape[axis_at] // shards_of)).reshape([-1 if axis == axis_at else 1 for axis in range(array.ndim)]) for axis_at in (source, target)]
    chosen = jax.random.permutation(stream_key, shards_of)[partner]
    strong = (owner == chosen) | (owner == (partner + shards_of // 2) % shards_of)
    return jnp.where(strong, factor * array, array)


def level_of(key, dims, split, least, top_value):
    gain, own = 1.0, jax.random.fold_in(key, 6)
    for position, parts in split:
        draws = jnp.exp(jax.random.uniform(jax.random.fold_in(own, position), (parts,), jnp.float32, least / len(split), top_value / len(split)))
        gain = gain * jnp.repeat(draws, dims[position] // parts).reshape([-1 if axis == position else 1 for axis in range(len(dims))])
    return gain


def centred(key, shape, scale, most, split=(), held_as=jnp.bfloat16):
    gain = level_of(key, shape, split, -0.22, 0.18) if split else 1.0
    values = jax.random.normal(key, shape, jnp.float32) * scale * gain
    return jnp.minimum(jnp.maximum(values, -most), most).astype(held_as)


def heavy_noise(stream_key, dims, spread, limit, shards, heavy, kind=jnp.bfloat16):
    result = spread * jax.random.normal(stream_key, dims, jnp.float32)
    if shards:
        result = result * level_of(stream_key, dims, shards, -0.22, 0.18)
    return jnp.clip(spiked(result, jax.random.fold_in(stream_key, 3), *heavy), -limit, limit).astype(kind)


def setup_inputs(seed: int = 0) -> dict:
    splits = jax.random.split(jax.random.key(seed), 9)
    bucket_of = draw_bucket_of(jax.random.fold_in(splits[8], 71), 0)
    lengths = draw_lengths(jax.random.fold_in(splits[8], 71), 0)
    counts = touch_ends(jax.random.randint(splits[2], (NB,), 256, 4097), jax.random.fold_in(splits[2], 1), 256, 4096).astype(jnp.int32)
    queries = draw_queries(jax.random.fold_in(splits[8], 71), 0)
    keys = draw_keys(jax.random.fold_in(splits[8], 71), 0)
    values = centred(splits[5], (TOKENS, HD), 1.0, 6.0, ((0, 32),))
    out_grad = heavy_noise(splits[6], (TOKENS, D), 1.0, 6.0, ((0, 32),), (0, 1, 32, 2.75))
    w_out = centred(splits[7], (HD, D), (max(D // 256, 1)) ** -0.5, 1.75, ((0, 8), (1, 4)))
    return dict(bucket_of=bucket_of, lengths=lengths, counts=counts, queries=queries, keys=keys, values=values, out_grad=out_grad, w_out=w_out)


def dot_nt(first_op, second_op):
    return lax.dot_general(first_op, second_op, (((1,), (1,)), ((), ())), preferred_element_type=jnp.float32)


def dot_tn(first_op, second_op):
    return lax.dot_general(first_op, second_op, (((0,), (0,)), ((), ())), preferred_element_type=jnp.float32)


def probabilities(query_rows, key_rows, keep_cols):
    scores = dot_nt(query_rows, key_rows) * (query_rows.shape[1] ** -0.5)
    scores = jnp.where(keep_cols[None, :], scores, -jnp.inf)
    row_top = jnp.max(scores, axis=1, keepdims=True)
    row_exp = jnp.exp(scores - row_top)
    return row_exp / jnp.sum(row_exp, axis=1, keepdims=True)


def item_grads(operands, keep_cols):
    query_rows, key_rows, value_rows, d_item = operands
    probs_full = probabilities(query_rows, key_rows, keep_cols)
    probs_low = probs_full.astype(jnp.bfloat16)
    attn_item = jnp.dot(probs_low, value_rows, preferred_element_type=jnp.float32).astype(jnp.bfloat16)
    row_delta = jnp.sum(d_item.astype(jnp.float32) * attn_item.astype(jnp.float32), axis=1, keepdims=True)
    dscore = (probs_full * (dot_nt(d_item, value_rows) - row_delta)).astype(jnp.bfloat16)
    factor = query_rows.shape[1] ** -0.5
    grad_q = (jnp.dot(dscore, key_rows, preferred_element_type=jnp.float32) * factor).astype(jnp.bfloat16)
    grad_k = (dot_tn(dscore, query_rows) * factor).astype(jnp.bfloat16)
    grad_v = dot_tn(probs_low, d_item).astype(jnp.bfloat16)
    return attn_item, grad_q, grad_k, grad_v


def split_heads(stacked, head_count):
    return stacked.reshape(SEQS, CAP, head_count, HEAD_DIM).transpose(0, 2, 1, 3).reshape(SEQS * head_count, CAP, HEAD_DIM)


def join_heads(stacked, head_count):
    return stacked.reshape(SEQS, head_count, CAP, HEAD_DIM).transpose(0, 2, 1, 3).reshape(SEQS * CAP, head_count * HEAD_DIM)


def reference(bucket_of, lengths, counts, queries, keys, values, out_grad, w_out):
    head_count = w_out.shape[0] // HEAD_DIM
    group_counts = counts[bucket_of].astype(jnp.float32)
    weights = group_counts / jnp.sum(group_counts)
    group_lengths = lengths[bucket_of]

    def one_group(running, group_index):
        row_first = (group_index * GTOK).astype(jnp.int32)
        slices = [lax.dynamic_slice_in_dim(source, row_first, GTOK, 0) for source in (queries, keys, values, out_grad)]
        keep_cols = jnp.arange(CAP, dtype=jnp.int32) < group_lengths[group_index]
        keep_rows = jnp.tile(keep_cols, SEQS)
        d_full = dot_nt(slices[3], w_out)
        d_attn = (d_full * keep_rows[:, None].astype(jnp.float32)).astype(jnp.bfloat16)
        operands = tuple(split_heads(source, head_count) for source in (slices[0], slices[1], slices[2], d_attn))
        attn_heads, grad_q, grad_k, grad_v = lax.map(partial(item_grads, keep_cols=keep_cols), operands)
        masked = join_heads(attn_heads, head_count) * keep_rows[:, None].astype(jnp.bfloat16)
        grad_part = dot_tn(masked, slices[3])
        return running + weights[group_index] * grad_part, (join_heads(grad_q, head_count), join_heads(grad_k, head_count), join_heads(grad_v, head_count))

    start_grad = jnp.zeros((w_out.shape[0], w_out.shape[1]), jnp.float32)
    summed_grad, stacked_grads = lax.scan(one_group, start_grad, jnp.arange(GROUPS, dtype=jnp.int32))
    grad_q, grad_k, grad_v = stacked_grads
    width = grad_q.shape[2]
    return grad_q.reshape(TOKENS, width), grad_k.reshape(TOKENS, width), grad_v.reshape(TOKENS, width), summed_grad
```

```python
import functools

import jax
import jax.numpy as jnp
from jax import lax
from jax.experimental import pallas as pl
from jax.experimental.pallas import tpu as pltpu
from jax.sharding import PartitionSpec as P

HEAD_DIM = 128
SEQS = 2
LAG = 2
MESH = pl.DeviceIdType.MESH
F32 = jnp.float32
BF16 = jnp.bfloat16


def dot(a, b, ca, cb):
    return lax.dot_general(a, b, (((ca,), (cb,)), ((), ())), preferred_element_type=F32)


def kernel(
    G, S, D, W, E,
    bucket_ref, length_ref, count_ref, q_ref, k_ref, v_ref, og_ref, w_ref,
    gq_ref, gk_ref, gv_ref, gw_ref,
    qh, kh, vh, dqs, dks, dvs, og, w, d_attn, attn_t, gs1, gr1, gown, gs2, gr2, gkeep, gs3, gr3,
    og_s, og_r, oz_s, oz_r, or_s, or_r, og_l, x_s, x_r, x_l, b_s, b_r, b_l,
    w0_s, w0_r, w_l, wy_s, wy_r, ws_s, ws_r, g1_s, g1_r, g2_s, g2_r, g3_s, g3_r,
):
    J = S // SEQS
    X = J // 2
    H = G // 2
    T = q_ref.shape[0]
    HD = q_ref.shape[1]
    L = J * T
    O = HD // S // W
    FM = 2 * O - E
    NM = FM + O
    NEAR = O - E
    BIG = 4 * O
    Dc = D // G
    scale = HEAD_DIM ** (-0.5)

    g = lax.axis_index("grp")
    s = lax.axis_index("sp")
    z, jx = s // X, s % X
    u, jz = z // 2, z % 2
    mid = (u + jz) % 2
    j = jz * X + jx
    h, c = g // 2, g % 2
    sibling = (h * 2 + 1 - c, s)

    def at(uu, mm, x):
        return (uu * 2 + (uu + mm) % 2) * X + x

    def foreign_of(mm):
        return E + mm * (FM - E)

    foreign = foreign_of(mid)
    mine = foreign + O
    theirs = foreign_of(1 - mid) + O

    def foreign_source(n, mm):
        far = mm * ((n + BIG - NEAR) // BIG)
        return 1 - far, n + mm * ((1 - far) * E - far * NEAR)

    def to_h(e):
        return ((h + e) % H * 2 + c, s)

    def seq_x(d):
        return (jx + d % X) % X

    def seq_from_x(d):
        return (jx - d % X + X) % X

    def seq_mid(d):
        return (mid + d // X) % 2

    def seq_row(d, x):
        return (jz + d // X) % 2 * X + x

    def seq_peer(d):
        return (g, at(u, seq_mid(d), seq_x(d)))

    across_mid = (g, at(1 - u, 1, jx))
    across_edge = (g, at(1 - u, 0, jx))

    peers = [seq_peer(d) for d in range(1, J)] + [to_h(e) for e in range(1, H)] + [sibling, across_mid]
    barrier = pltpu.get_barrier_semaphore()
    for peer in peers:
        pl.semaphore_signal(barrier, inc=1, device_id=peer, device_id_type=MESH)

    @pl.when(mid == 1)
    def _():
        pl.semaphore_signal(barrier, inc=1, device_id=across_edge, device_id_type=MESH)

    pl.semaphore_wait(barrier, len(peers) + mid)

    def remote(src, dst, ss, rs, dev):
        return pltpu.make_async_remote_copy(
            src_ref=src, dst_ref=dst, send_sem=ss, recv_sem=rs, device_id=dev, device_id_type=MESH
        )

    def col_of(ch, mm, x):
        first = foreign_of(mm)
        own = (ch + BIG - first) // BIG
        source_mid, piece_at = foreign_source(ch, mm)
        source = own * at(u, mm, x) + (1 - own) * at(1 - u, source_mid, x)
        return pl.multiple_of((source * O + own * (ch - first) + (1 - own) * piece_at) * W, W)

    def rows(jj):
        return pl.ds(pl.multiple_of(jj * T, T), T)

    xs = ((q_ref, qh), (k_ref, kh), (v_ref, vh))
    bs = ((dqs, gq_ref), (dks, gk_ref), (dvs, gv_ref))

    def w_rows(m):
        return w_ref.at[pl.ds(m * W, W)]

    def w0_copy(m):
        target_mid, n = (1 - mid, m) if m < E else (1, m - E)
        n = (1 - mid) * (NEAR + m) + mid * n
        return remote(w_rows(m), w.at[n, g], w0_s.at[m], w0_r.at[n], (g, at(1 - u, target_mid, jx)))

    def w0_arrival(n):
        return remote(w.at[n, g], w.at[n, g], w0_s.at[0], w0_r.at[n], across_mid)

    def wy_copy(src, ch, e):
        return remote(src, w.at[ch, g], wy_s.at[ch, e], wy_r.at[ch, e], to_h(e))

    def ws_own(src, ch):
        return remote(src, w.at[ch, g], ws_s.at[ch, 0], ws_r.at[ch, 0], sibling)

    def ws_copy(ch, e):
        src = (h - e + H) % H * 2 + c
        return remote(w.at[ch, src], w.at[ch, src], ws_s.at[ch, e], ws_r.at[ch, e], sibling)

    def wy_arrival(ch, e):
        src = (h - e + H) % H * 2 + c
        return remote(w.at[ch, src], w.at[ch, src], wy_s.at[ch, e], wy_r.at[ch, e], to_h(e))

    def ws_arrival(ch, e):
        src = (h - e + H) % H * 2 + 1 - c
        return remote(w.at[ch, src], w.at[ch, src], ws_s.at[ch, e], ws_r.at[ch, e], sibling)

    mate = (1 - jz) * X + jx

    def og_x_peer(e):
        return (g, u * J + jz * X + (jx + e) % X)

    def piece(jj, p):
        return og.at[pl.ds(pl.multiple_of(jj * T + p * (T // 2), T // 2), T // 2)]

    def og_z(p):
        src = og_ref.at[pl.ds(p * (T // 2), T // 2)]
        return remote(src, piece(j, p), oz_s.at[p], oz_r.at[p], (g, u * J + mate))

    def og_z_arrival(p):
        src = og_ref.at[pl.ds(p * (T // 2), T // 2)]
        return remote(src, piece(mate, p), oz_s.at[p], oz_r.at[p], (g, u * J + mate))

    def og_x(e):
        return remote(og_ref, og.at[rows(j)], og_s.at[e], og_r.at[e], og_x_peer(e))

    def og_x_arrival(e):
        src = rows(jz * X + (jx - e + X) % X)
        return remote(og_ref, og.at[src], og_s.at[e], og_r.at[e], og_x_peer(e))

    def og_relay(e, p):
        block = piece(mate, p)
        return remote(block, block, or_s.at[e, p], or_r.at[e, p], og_x_peer(e))

    def og_relay_arrival(e, p):
        block = piece((1 - jz) * X + (jx - e + X) % X, p)
        return remote(block, block, or_s.at[e, p], or_r.at[e, p], og_x_peer(e))

    def x_copy(ch, i, d):
        src, dst = xs[i]
        cols = pl.ds(col_of(ch, seq_mid(d), seq_x(d)), W)
        return remote(
            src.at[:, cols], dst.at[ch, rows(j)], x_s.at[ch, i, d], x_r.at[ch, i, d], seq_peer(d)
        )

    def x_arrival(ch, i, d):
        src, dst = xs[i]
        return remote(
            src.at[:, pl.ds(0, W)], dst.at[ch, rows(seq_row(d, seq_from_x(d)))],
            x_s.at[ch, i, d], x_r.at[ch, i, d], seq_peer(d),
        )

    def x_local(ch, i):
        src, dst = xs[i]
        return pltpu.make_async_copy(
            src.at[:, pl.ds(col_of(ch, mid, jx), W)], dst.at[ch, rows(j)], x_l.at[ch, i]
        )

    def b_copy(ch, i, d):
        src, dst = bs[i]
        return remote(
            src.at[ch, rows(seq_row(d, seq_x(d)))], dst.at[:, pl.ds(col_of(ch, mid, jx), W)],
            b_s.at[ch, i, d], b_r.at[ch, i, d], seq_peer(d),
        )

    def b_arrival(ch, i, d):
        src, dst = bs[i]
        return remote(
            src.at[ch, rows(j)], dst.at[:, pl.ds(col_of(ch, seq_mid(d), seq_from_x(d)), W)],
            b_s.at[ch, i, d], b_r.at[ch, i, d], seq_peer(d),
        )

    def b_local(ch, i):
        src, dst = bs[i]
        return pltpu.make_async_copy(
            src.at[ch, rows(j)], dst.at[:, pl.ds(col_of(ch, mid, jx), W)], b_l.at[ch, i]
        )

    og_own = pltpu.make_async_copy(og_ref, og.at[rows(j)], og_l)

    def w_local(m):
        return pltpu.make_async_copy(w_rows(m), w.at[foreign + m, g], w_l.at[m])

    def g1_copy(ch):
        return remote(gs1.at[ch], gr1.at[ch], g1_s.at[ch], g1_r.at[ch], sibling)

    def g2_copy(ch, e):
        return remote(gs2.at[ch, e - 1], gr2.at[ch, e - 1], g2_s.at[ch, e], g2_r.at[ch, e], to_h(e))

    def g3_copy(n):
        source_mid, m = foreign_source(n, mid)
        return remote(
            gs3.at[n], gr3.at[m], g3_s.at[n], g3_r.at[m], (g, at(1 - u, source_mid, jx))
        )

    def g3_arrival(m):
        return remote(gr3.at[m], gr3.at[m], g3_s.at[0], g3_r.at[m], across_mid)

    @pl.when(mid == 1)
    def _():
        for m in range(O):
            w0_copy(m).start()

    og_z(0).start()
    og_z(1).start()
    for e in range(1, X):
        og_x(e).start()
    for m in range(O):
        for e in range(1, H):
            wy_copy(w_rows(m), foreign + m, e).start()
        ws_own(w_rows(m), foreign + m).start()
        w_local(m).start()
    og_own.start()

    def send_chunk(ch, carry):
        @pl.when(ch < theirs)
        def _():
            for i in range(3):
                for d in range(X, J):
                    x_copy(ch, i, d).start()

        @pl.when(ch < mine)
        def _():
            for i in range(3):
                for d in range(1, X):
                    x_copy(ch, i, d).start()
                x_local(ch, i).start()

        return carry

    for ch in range(O):
        @pl.when(mid == 0)
        def _():
            w0_copy(ch).start()

        if ch == 0:
            send_chunk(0, 0)

    def relay_w0(n):
        w0_arrival(n).wait_recv()
        for e in range(1, H):
            wy_copy(w.at[n, g], n, e).start()
        ws_own(w.at[n, g], n).start()

    def forward_w(ch):
        for e in range(1, H):
            wy_arrival(ch, e).wait_recv()
            ws_copy(ch, e).start()

    for p in range(2):
        og_z_arrival(p).wait_recv()
        for e in range(1, X):
            og_relay(e, p).start()
    lax.fori_loop(1, NM, send_chunk, 0)
    for n in range(min(2, FM)):
        @pl.when(n < foreign)
        def _():
            relay_w0(n)
    forward_w(0)
    for m in range(O):
        w_local(m).wait()
    og_own.wait()
    for e in range(1, X):
        og_x_arrival(e).wait_recv()
        og_relay_arrival(e, 0).wait_recv()
        og_relay_arrival(e, 1).wait_recv()

    seq_len = length_ref[bucket_ref[g]]
    total = count_ref[bucket_ref[0]]
    for other in range(1, G):
        total = total + count_ref[bucket_ref[other]]
    weight = jnp.full((1, 1), count_ref[bucket_ref[g]], jnp.int32).astype(F32) / jnp.full(
        (1, 1), total, jnp.int32
    ).astype(F32)
    keep_key = lax.broadcasted_iota(jnp.int32, (L, 1), 0) < seq_len
    keep_col = lax.broadcasted_iota(jnp.int32, (1, L), 1) < seq_len

    def compute(ch):
        for i in range(3):
            x_local(ch, i).wait()
            for d in range(1, J):
                x_arrival(ch, i, d).wait_recv()
        for e in range(H):
            ws_arrival(ch, e).wait_recv()
        acc = dot(og[:, 0:Dc], w[ch, 0], 1, 1)
        for gg in range(1, G):
            acc = acc + dot(og[:, gg * Dc:(gg + 1) * Dc], w[ch, gg], 1, 1)
        d_attn[...] = jnp.where(keep_key, acc, 0.0).astype(BF16)

        for n in range(W // HEAD_DIM):
            lanes = slice(n * HEAD_DIM, (n + 1) * HEAD_DIM)
            q = qh[ch, :, lanes]
            k = kh[ch, :, lanes]
            v = vh[ch, :, lanes]
            do = d_attn[:, lanes]
            scores = jnp.where(keep_key, dot(k, q, 1, 1) * scale, -1e30)
            top = jnp.max(scores, axis=0, keepdims=True)
            ex = jnp.exp(scores - top)
            probs = ex * (1.0 / jnp.sum(ex, axis=0, keepdims=True))
            low = probs.astype(BF16)
            attn = dot(v, low, 0, 0)
            attn_t[lanes, :] = jnp.where(keep_col, attn, 0.0).astype(BF16)
            dp = dot(v, do, 1, 1)
            delta = jnp.sum(probs * dp, axis=0, keepdims=True)
            ds = (probs * (dp - delta)).astype(BF16)
            dvs[ch, :, lanes] = dot(low, do, 1, 0).astype(BF16)
            dks[ch, :, lanes] = (dot(ds, q, 1, 0) * scale).astype(BF16)
            dqs[ch, :, lanes] = (dot(k, ds, 0, 0) * scale).T.astype(BF16)
        for i in range(3):
            for d in range(1, J):
                b_copy(ch, i, d).start()
            b_local(ch, i).start()

        @pl.when(ch + 1 < mine)
        def _():
            forward_w(ch + 1)

        for hh in range(H):
            low_c, high_c = (
                dot(attn_t[...], og[:, gg * Dc:(gg + 1) * Dc], 1, 0) * weight
                for gg in (2 * hh, 2 * hh + 1)
            )
            gown[ch, hh] = jnp.where(c == 0, low_c, high_c)
            gs1[ch, hh] = jnp.where(c == 0, high_c, low_c).astype(BF16)
        g1_copy(ch).start()

    def across_groups(ch):
        g1_copy(ch).wait_recv()
        for e in range(1, H):
            to = (h + e) % H
            gs2[ch, e - 1] = (gown[ch, to] + gr1[ch, to].astype(F32)).astype(BF16)
            g2_copy(ch, e).start()
        gkeep[ch] = gown[ch, h] + gr1[ch, h].astype(F32)

    def across_halves(ch):
        part = gkeep[ch]
        for e in range(1, H):
            g2_copy(ch, e).wait_recv()
            part = part + gr2[ch, e - 1].astype(F32)

        @pl.when(ch < foreign)
        def _():
            gs3[ch] = part.astype(BF16)
            g3_copy(ch).start()

        @pl.when(ch >= foreign)
        def _():
            gkeep[ch] = part

    def step(n, carry):
        @pl.when((n >= 1) & (n + 1 < foreign))
        def _():
            relay_w0(n + 1)

        @pl.when(n < mine)
        def _():
            compute(n)

        @pl.when((n >= 1) & (n < mine + 1))
        def _():
            across_groups(n - 1)

        @pl.when((n >= LAG) & (n < mine + LAG))
        def _():
            across_halves(n - LAG)

        return carry

    lax.fori_loop(0, mine + LAG, step, 0)

    for m in range(O):
        g3_arrival(m).wait_recv()
        gw_ref[m * W:(m + 1) * W, :] = gkeep[foreign + m] + gr3[m].astype(F32)

    og_z(0).wait_send()
    og_z(1).wait_send()
    for e in range(1, X):
        og_x(e).wait_send()
        og_relay(e, 0).wait_send()
        og_relay(e, 1).wait_send()
    for m in range(O):
        w0_copy(m).wait_send()

    def drain(ch, carry):
        @pl.when(ch < foreign)
        def _():
            g3_copy(ch).wait_send()

        @pl.when(ch < mine)
        def _():
            ws_own(w.at[ch, g], ch).wait_send()
            for e in range(1, H):
                ws_copy(ch, e).wait_send()
                wy_copy(w.at[ch, g], ch, e).wait_send()
                g2_copy(ch, e).wait_send()
            g1_copy(ch).wait_send()
            for i in range(3):
                b_local(ch, i).wait()
                for d in range(1, J):
                    b_copy(ch, i, d).wait_send()
                for d in range(1, X):
                    x_copy(ch, i, d).wait_send()
                    b_arrival(ch, i, d).wait_recv()

        @pl.when(ch < theirs)
        def _():
            for i in range(3):
                for d in range(X, J):
                    x_copy(ch, i, d).wait_send()
                    b_arrival(ch, i, d).wait_recv()

        return carry

    lax.fori_loop(0, NM, drain, 0)


def solution(mesh):
    G, S = mesh.shape["grp"], mesh.shape["sp"]
    J, H = S // SEQS, G // 2
    X = J // 2

    def shards(bucket_of, lengths, counts, queries, keys, values, out_grad, w_out):
        T, HD = queries.shape
        D = out_grad.shape[1]
        L, R, Dc = J * T, HD // S, D // G
        W = 256 if R % 256 == 0 else 128
        O = R // W
        E = O // 2
        NM = 3 * O - E
        FM = NM - O
        dma = pltpu.SemaphoreType.DMA
        head = pltpu.VMEM((NM, L, W), BF16)
        smem = pl.BlockSpec(memory_space=pltpu.SMEM)
        hbm = pl.BlockSpec(memory_space=pltpu.HBM)
        grad = jax.ShapeDtypeStruct((T, HD), BF16)
        return pl.pallas_call(
            functools.partial(kernel, G, S, D, W, E),
            out_shape=(grad, grad, grad, jax.ShapeDtypeStruct((R, Dc), F32)),
            in_specs=[smem] * 3 + [hbm] * 5,
            out_specs=(hbm, hbm, hbm, pl.BlockSpec(memory_space=pltpu.VMEM)),
            scratch_shapes=[head] * 6 + [
                pltpu.VMEM((L, D), BF16),
                pltpu.VMEM((NM, G, W, Dc), BF16),
                pltpu.VMEM((L, W), BF16),
                pltpu.VMEM((W, L), BF16),
                pltpu.VMEM((NM, H, W, Dc), BF16),
                pltpu.VMEM((NM, H, W, Dc), BF16),
                pltpu.VMEM((NM, H, W, Dc), F32),
                pltpu.VMEM((NM, H - 1, W, Dc), BF16),
                pltpu.VMEM((NM, H - 1, W, Dc), BF16),
                pltpu.VMEM((NM, W, Dc), F32),
                pltpu.VMEM((FM, W, Dc), BF16),
                pltpu.VMEM((O, W, Dc), BF16),
                dma((X,)), dma((X,)), dma((2,)), dma((2,)), dma((X, 2)), dma((X, 2)), dma(()),
                dma((NM, 3, J)), dma((NM, 3, J)), dma((NM, 3)),
                dma((NM, 3, J)), dma((NM, 3, J)), dma((NM, 3)),
                dma((O,)), dma((FM,)), dma((O,)),
                dma((NM, H)), dma((NM, H)), dma((NM, H)), dma((NM, H)),
                dma((NM,)), dma((NM,)), dma((NM, H)), dma((NM, H)),
                dma((FM,)), dma((O,)),
            ],
            compiler_params=pltpu.CompilerParams(
                collective_id=0, has_side_effects=True, vmem_limit_bytes=62 * 1024 * 1024
            ),
        )(bucket_of, lengths, counts, queries, keys, values, out_grad, w_out)

    rows = P(("grp", "sp"), None)
    return jax.shard_map(
        shards,
        mesh=mesh,
        in_specs=(P(), P(), P(), rows, rows, rows, rows, P("sp", "grp")),
        out_specs=(rows, rows, rows, P("sp", "grp")),
        check_vma=False,
    )
```

```python
import functools

import jax
import jax.numpy as jnp
from jax import lax
from jax.experimental import pallas as pl
from jax.experimental.pallas import tpu as pltpu
from jax.sharding import PartitionSpec as P

HEAD_DIM = 128
SEQS = 2
LAG = 2
PARTS = 2
MESH = pl.DeviceIdType.MESH
F32 = jnp.float32
BF16 = jnp.bfloat16


def dot(a, b, ca, cb):
    return lax.dot_general(a, b, (((ca,), (cb,)), ((), ())), preferred_element_type=F32)


def schedule(role, O, E, NM):
    w0 = [("w0", m) for m in range(O)]
    if role == 1:
        w0 = w0[E:] + w0[:E]
    first = [("ogz", 0), ("ogz", 1), ("ogx", 0), ("wy", 0)]
    relays = [("ogr", 0), ("ogr", 1)]
    last = [("relay", 0), ("relay", 1), ("fwd", 0)]
    rest = [(kind, ch) for ch in range(1, NM) for kind in ("x1", "x3", "x2")]
    if role == 0:
        return first + w0[:1] + [("x1", 0), ("x3", 0), ("x2", 0)] + w0[1:] + relays + rest + last
    return w0 + first + [("x1", 0), ("x3", 0), ("x2", 0)] + relays + rest + last


def kernel(
    G, S, D, W, E,
    bucket_ref, length_ref, count_ref, q_ref, k_ref, v_ref, og_ref, w_ref,
    gq_ref, gk_ref, gv_ref, gw_ref,
    qh, kh, vh, dqs, dks, dvs, og, w, d_attn, attn_t, gs1, gr1, gown, gs2, gr2, gkeep, gs3, gr3,
    og_s, og_r, oz_s, oz_r, or_s, or_r, og_l, x_s, x_r, x_l, b_s, b_r, b_l,
    w0_s, w0_r, w_l, wy_s, wy_r, ws_s, ws_r, g1_s, g1_r, g2_s, g2_r, g3_s, g3_r,
):
    J = S // SEQS
    X = J // 2
    H = G // 2
    T = q_ref.shape[0]
    HD = q_ref.shape[1]
    L = J * T
    O = HD // S // W
    FM = 2 * O - E
    NM = FM + O
    NEAR = O - E
    BIG = 4 * O
    Dc = D // G
    scale = HEAD_DIM ** (-0.5)

    g = lax.axis_index("grp")
    s = lax.axis_index("sp")
    z, jx = s // X, s % X
    u, jz = z // 2, z % 2
    mid = (u + jz) % 2
    j = jz * X + jx
    h, c = g // 2, g % 2
    sibling = (h * 2 + 1 - c, s)

    def at(uu, mm, x):
        return (uu * 2 + (uu + mm) % 2) * X + x

    def foreign_of(mm):
        return E + mm * (FM - E)

    foreign = foreign_of(mid)
    mine = foreign + O
    theirs = foreign_of(1 - mid) + O

    def foreign_source(n, mm):
        far = mm * ((n + BIG - NEAR) // BIG)
        return 1 - far, n + mm * ((1 - far) * E - far * NEAR)

    def to_h(e):
        return ((h + e) % H * 2 + c, s)

    def seq_x(d):
        return (jx + d % X) % X

    def seq_from_x(d):
        return (jx - d % X + X) % X

    def seq_mid(d):
        return (mid + d // X) % 2

    def seq_row(d, x):
        return (jz + d // X) % 2 * X + x

    def seq_peer(d):
        return (g, at(u, seq_mid(d), seq_x(d)))

    across_mid = (g, at(1 - u, 1, jx))
    across_edge = (g, at(1 - u, 0, jx))

    peers = [seq_peer(d) for d in range(1, J)] + [to_h(e) for e in range(1, H)] + [sibling, across_mid]
    barrier = pltpu.get_barrier_semaphore()
    for peer in peers:
        pl.semaphore_signal(barrier, inc=1, device_id=peer, device_id_type=MESH)

    @pl.when(mid == 1)
    def _():
        pl.semaphore_signal(barrier, inc=1, device_id=across_edge, device_id_type=MESH)

    def remote(src, dst, ss, rs, dev):
        return pltpu.make_async_remote_copy(
            src_ref=src, dst_ref=dst, send_sem=ss, recv_sem=rs, device_id=dev, device_id_type=MESH
        )

    def col_of(ch, mm, x):
        first = foreign_of(mm)
        own = (ch + BIG - first) // BIG
        source_mid, piece_at = foreign_source(ch, mm)
        source = own * at(u, mm, x) + (1 - own) * at(1 - u, source_mid, x)
        return pl.multiple_of((source * O + own * (ch - first) + (1 - own) * piece_at) * W, W)

    def rows(jj):
        return pl.ds(pl.multiple_of(jj * T, T), T)

    xs = ((q_ref, qh), (k_ref, kh), (v_ref, vh))
    bs = ((dqs, gq_ref), (dks, gk_ref), (dvs, gv_ref))

    def w_rows(m):
        return w_ref.at[pl.ds(m * W, W)]

    def w0_copy(m):
        target_mid, n = (1 - mid, m) if m < E else (1, m - E)
        n = (1 - mid) * (NEAR + m) + mid * n
        return remote(w_rows(m), w.at[n, g], w0_s.at[m], w0_r.at[n], (g, at(1 - u, target_mid, jx)))

    def w0_arrival(n):
        return remote(w.at[n, g], w.at[n, g], w0_s.at[0], w0_r.at[n], across_mid)

    def wy_copy(src, ch, e):
        return remote(src, w.at[ch, g], wy_s.at[ch, e], wy_r.at[ch, e], to_h(e))

    def ws_own(src, ch):
        return remote(src, w.at[ch, g], ws_s.at[ch, 0], ws_r.at[ch, 0], sibling)

    def ws_copy(ch, e):
        src = (h - e + H) % H * 2 + c
        return remote(w.at[ch, src], w.at[ch, src], ws_s.at[ch, e], ws_r.at[ch, e], sibling)

    def wy_arrival(ch, e):
        src = (h - e + H) % H * 2 + c
        return remote(w.at[ch, src], w.at[ch, src], wy_s.at[ch, e], wy_r.at[ch, e], to_h(e))

    def ws_arrival(ch, e):
        src = (h - e + H) % H * 2 + 1 - c
        return remote(w.at[ch, src], w.at[ch, src], ws_s.at[ch, e], ws_r.at[ch, e], sibling)

    mate = (1 - jz) * X + jx

    def og_x_peer(e):
        return (g, u * J + jz * X + (jx + e) % X)

    def piece(jj, p):
        return og.at[pl.ds(pl.multiple_of(jj * T + p * (T // 2), T // 2), T // 2)]

    def og_z(p):
        src = og_ref.at[pl.ds(p * (T // 2), T // 2)]
        return remote(src, piece(j, p), oz_s.at[p], oz_r.at[p], (g, u * J + mate))

    def og_z_arrival(p):
        src = og_ref.at[pl.ds(p * (T // 2), T // 2)]
        return remote(src, piece(mate, p), oz_s.at[p], oz_r.at[p], (g, u * J + mate))

    def og_x(e):
        return remote(og_ref, og.at[rows(j)], og_s.at[e], og_r.at[e], og_x_peer(e))

    def og_x_arrival(e):
        src = rows(jz * X + (jx - e + X) % X)
        return remote(og_ref, og.at[src], og_s.at[e], og_r.at[e], og_x_peer(e))

    def og_relay(e, p):
        block = piece(mate, p)
        return remote(block, block, or_s.at[e, p], or_r.at[e, p], og_x_peer(e))

    def og_relay_arrival(e, p):
        block = piece((1 - jz) * X + (jx - e + X) % X, p)
        return remote(block, block, or_s.at[e, p], or_r.at[e, p], og_x_peer(e))

    def x_copy(ch, i, d):
        src, dst = xs[i]
        cols = pl.ds(col_of(ch, seq_mid(d), seq_x(d)), W)
        return remote(
            src.at[:, cols], dst.at[ch, rows(j)], x_s.at[ch, i, d], x_r.at[ch, i, d], seq_peer(d)
        )

    def x_arrival(ch, i, d):
        src, dst = xs[i]
        return remote(
            src.at[:, pl.ds(0, W)], dst.at[ch, rows(seq_row(d, seq_from_x(d)))],
            x_s.at[ch, i, d], x_r.at[ch, i, d], seq_peer(d),
        )

    def x_local(ch, i):
        src, dst = xs[i]
        return pltpu.make_async_copy(
            src.at[:, pl.ds(col_of(ch, mid, jx), W)], dst.at[ch, rows(j)], x_l.at[ch, i]
        )

    def b_copy(ch, i, d):
        src, dst = bs[i]
        return remote(
            src.at[ch, rows(seq_row(d, seq_x(d)))], dst.at[:, pl.ds(col_of(ch, mid, jx), W)],
            b_s.at[ch, i, d], b_r.at[ch, i, d], seq_peer(d),
        )

    def b_arrival(ch, i, d):
        src, dst = bs[i]
        return remote(
            src.at[ch, rows(j)], dst.at[:, pl.ds(col_of(ch, seq_mid(d), seq_from_x(d)), W)],
            b_s.at[ch, i, d], b_r.at[ch, i, d], seq_peer(d),
        )

    def b_local(ch, i):
        src, dst = bs[i]
        return pltpu.make_async_copy(
            src.at[ch, rows(j)], dst.at[:, pl.ds(col_of(ch, mid, jx), W)], b_l.at[ch, i]
        )

    og_own = pltpu.make_async_copy(og_ref, og.at[rows(j)], og_l)

    def w_local(m):
        return pltpu.make_async_copy(w_rows(m), w.at[foreign + m, g], w_l.at[m])

    def g1_copy(ch):
        return remote(gs1.at[ch], gr1.at[ch], g1_s.at[ch], g1_r.at[ch], sibling)

    def g2_copy(ch, e):
        return remote(gs2.at[ch, e - 1], gr2.at[ch, e - 1], g2_s.at[ch, e], g2_r.at[ch, e], to_h(e))

    def g3_copy(n):
        source_mid, m = foreign_source(n, mid)
        return remote(
            gs3.at[n], gr3.at[m], g3_s.at[n], g3_r.at[m], (g, at(1 - u, source_mid, jx))
        )

    def g3_arrival(m):
        return remote(gr3.at[m], gr3.at[m], g3_s.at[0], g3_r.at[m], across_mid)

    og_own.start()
    for m in range(O):
        w_local(m).start()

    def local_chunk(ch, carry):
        for i in range(3):
            x_local(ch, i).start()
        return carry

    lax.fori_loop(0, mine, local_chunk, 0)
    pl.semaphore_wait(barrier, len(peers) + mid)

    def relay_w0(n):
        w0_arrival(n).wait_recv()
        for e in range(1, H):
            wy_copy(w.at[n, g], n, e).start()
        ws_own(w.at[n, g], n).start()

    def forward_w(ch):
        for e in range(1, H):
            wy_arrival(ch, e).wait_recv()
            ws_copy(ch, e).start()

    def issue(kind, n, role):
        theirs_n = E + (1 - role) * (FM - E) + O
        mine_n = E + role * (FM - E) + O
        first = mine_n - O
        if kind == "w0" and n < O:
            w0_copy(n).start()
        elif kind == "ogz":
            og_z(n).start()
        elif kind == "ogx":
            for e in range(1, X):
                og_x(e).start()
        elif kind == "ogr":
            og_z_arrival(n).wait_recv()
            for e in range(1, X):
                og_relay(e, n).start()
        elif kind == "wy":
            for m in range(O):
                for e in range(1, H):
                    wy_copy(w_rows(m), first + m, e).start()
                ws_own(w_rows(m), first + m).start()
        elif kind == "x1" and n < theirs_n:
            for i in range(3):
                x_copy(n, i, X).start()
        elif kind == "x3" and n < theirs_n:
            for i in range(3):
                for d in range(X + 1, J):
                    x_copy(n, i, d).start()
        elif kind == "x2" and n < mine_n:
            for i in range(3):
                for d in range(1, X):
                    x_copy(n, i, d).start()
        elif kind == "relay" and n < first:
            relay_w0(n)
        elif kind == "fwd":
            forward_w(n)

    for role in range(2):
        @pl.when(mid == role)
        def _():
            for kind, n in schedule(role, O, E, NM):
                issue(kind, n, role)

    for m in range(O):
        w_local(m).wait()
    og_own.wait()
    for e in range(1, X):
        og_x_arrival(e).wait_recv()
        og_relay_arrival(e, 0).wait_recv()
        og_relay_arrival(e, 1).wait_recv()

    seq_len = length_ref[bucket_ref[g]]
    total = count_ref[bucket_ref[0]]
    for other in range(1, G):
        total = total + count_ref[bucket_ref[other]]
    weight = jnp.full((1, 1), count_ref[bucket_ref[g]], jnp.int32).astype(F32) / jnp.full(
        (1, 1), total, jnp.int32
    ).astype(F32)
    keep_key = lax.broadcasted_iota(jnp.int32, (L, 1), 0) < seq_len
    keep_col = lax.broadcasted_iota(jnp.int32, (1, L), 1) < seq_len

    def compute(ch):
        for i in range(3):
            x_local(ch, i).wait()
            for d in range(1, J):
                x_arrival(ch, i, d).wait_recv()
        for e in range(H):
            ws_arrival(ch, e).wait_recv()
        acc = dot(og[:, 0:Dc], w[ch, 0], 1, 1)
        for gg in range(1, G):
            acc = acc + dot(og[:, gg * Dc:(gg + 1) * Dc], w[ch, gg], 1, 1)
        d_attn[...] = jnp.where(keep_key, acc, 0.0).astype(BF16)

        @pl.when(ch >= 1)
        def _():
            across_groups(ch - 1)

        for n in range(W // HEAD_DIM):
            lanes = slice(n * HEAD_DIM, (n + 1) * HEAD_DIM)
            q = qh[ch, :, lanes]
            k = kh[ch, :, lanes]
            v = vh[ch, :, lanes]
            do = d_attn[:, lanes]
            scores = jnp.where(keep_key, dot(k, q, 1, 1) * scale, -1e30)
            top = jnp.max(scores, axis=0, keepdims=True)
            ex = jnp.exp(scores - top)
            probs = ex * (1.0 / jnp.sum(ex, axis=0, keepdims=True))
            low = probs.astype(BF16)
            attn = dot(v, low, 0, 0)
            attn_t[lanes, :] = jnp.where(keep_col, attn, 0.0).astype(BF16)
            dp = dot(v, do, 1, 1)
            delta = jnp.sum(probs * dp, axis=0, keepdims=True)
            ds = (probs * (dp - delta)).astype(BF16)
            dvs[ch, :, lanes] = dot(low, do, 1, 0).astype(BF16)
            dks[ch, :, lanes] = (dot(ds, q, 1, 0) * scale).astype(BF16)
            dqs[ch, :, lanes] = (dot(k, ds, 0, 0) * scale).T.astype(BF16)
        for i in range(3):
            for d in range(1, J):
                b_copy(ch, i, d).start()
            b_local(ch, i).start()

        @pl.when(ch + 1 < mine)
        def _():
            forward_w(ch + 1)

        @pl.when(ch >= LAG)
        def _():
            across_halves(ch - LAG)

        for hh in range(H):
            low_c, high_c = (
                dot(attn_t[...], og[:, gg * Dc:(gg + 1) * Dc], 1, 0) * weight
                for gg in (2 * hh, 2 * hh + 1)
            )
            gown[ch, hh] = jnp.where(c == 0, low_c, high_c)
            gs1[ch, hh] = jnp.where(c == 0, high_c, low_c).astype(BF16)
        g1_copy(ch).start()

    def across_groups(ch):
        g1_copy(ch).wait_recv()
        for e in range(1, H):
            to = (h + e) % H
            gs2[ch, e - 1] = (gown[ch, to] + gr1[ch, to].astype(F32)).astype(BF16)
            g2_copy(ch, e).start()
        gkeep[ch] = gown[ch, h] + gr1[ch, h].astype(F32)

    def across_halves(ch):
        part = gkeep[ch]
        for e in range(1, H):
            g2_copy(ch, e).wait_recv()
            part = part + gr2[ch, e - 1].astype(F32)

        @pl.when(ch < foreign)
        def _():
            gs3[ch] = part.astype(BF16)
            g3_copy(ch).start()

        @pl.when(ch >= foreign)
        def _():
            gkeep[ch] = part

    def step(n, carry):
        @pl.when((n >= 1) & (n + 1 < foreign))
        def _():
            relay_w0(n + 1)

        compute(n)
        return carry

    lax.fori_loop(0, mine, step, 0)
    across_groups(mine - 1)
    for n in range(LAG, 0, -1):
        @pl.when(mine >= n)
        def _():
            across_halves(mine - n)

    for m in range(O):
        g3_arrival(m).wait_recv()
        gw_ref[m * W:(m + 1) * W, :] = gkeep[foreign + m] + gr3[m].astype(F32)

    og_z(0).wait_send()
    og_z(1).wait_send()
    for e in range(1, X):
        og_x(e).wait_send()
        og_relay(e, 0).wait_send()
        og_relay(e, 1).wait_send()
    for m in range(O):
        w0_copy(m).wait_send()

    def drain(ch, carry):
        @pl.when(ch < foreign)
        def _():
            g3_copy(ch).wait_send()

        @pl.when(ch < mine)
        def _():
            ws_own(w.at[ch, g], ch).wait_send()
            for e in range(1, H):
                ws_copy(ch, e).wait_send()
                wy_copy(w.at[ch, g], ch, e).wait_send()
                g2_copy(ch, e).wait_send()
            g1_copy(ch).wait_send()
            for i in range(3):
                b_local(ch, i).wait()
                for d in range(1, J):
                    b_copy(ch, i, d).wait_send()
                for d in range(1, X):
                    x_copy(ch, i, d).wait_send()
                    b_arrival(ch, i, d).wait_recv()

        @pl.when(ch < theirs)
        def _():
            for i in range(3):
                for d in range(X, J):
                    x_copy(ch, i, d).wait_send()
                    b_arrival(ch, i, d).wait_recv()

        return carry

    lax.fori_loop(0, NM, drain, 0)


def store(*refs):
    sems = refs[-1]
    copies = []
    for i in range(4):
        rows = refs[i].shape[0] // PARTS
        for n in range(PARTS):
            part = pl.ds(n * rows, rows)
            copies.append(pltpu.make_async_copy(refs[i].at[part], refs[4 + i].at[part], sems.at[i, n]))
    for copy in copies:
        copy.start()
    for copy in copies:
        copy.wait()


def solution(mesh):
    G, S = mesh.shape["grp"], mesh.shape["sp"]
    J, H = S // SEQS, G // 2
    X = J // 2

    def shards(bucket_of, lengths, counts, queries, keys, values, out_grad, w_out):
        T, HD = queries.shape
        D = out_grad.shape[1]
        L, R, Dc = J * T, HD // S, D // G
        W = 256 if R % 256 == 0 else 128
        O = R // W
        E = O // 2
        NM = 3 * O - E
        FM = NM - O
        dma = pltpu.SemaphoreType.DMA
        head = pltpu.VMEM((NM, L, W), BF16)
        smem = pl.BlockSpec(memory_space=pltpu.SMEM)
        hbm = pl.BlockSpec(memory_space=pltpu.HBM)
        grad = jax.ShapeDtypeStruct((T, HD), BF16)
        held = pl.pallas_call(
            functools.partial(kernel, G, S, D, W, E),
            out_shape=(pltpu.VMEM((T, HD), BF16),) * 3 + (pltpu.VMEM((R, Dc), F32),),
            in_specs=[smem] * 3 + [hbm] * 5,
            out_specs=(pl.BlockSpec(memory_space=pltpu.VMEM),) * 4,
            scratch_shapes=[head] * 6 + [
                pltpu.VMEM((L, D), BF16),
                pltpu.VMEM((NM, G, W, Dc), BF16),
                pltpu.VMEM((L, W), BF16),
                pltpu.VMEM((W, L), BF16),
                pltpu.VMEM((NM, H, W, Dc), BF16),
                pltpu.VMEM((NM, H, W, Dc), BF16),
                pltpu.VMEM((NM, H, W, Dc), F32),
                pltpu.VMEM((NM, H - 1, W, Dc), BF16),
                pltpu.VMEM((NM, H - 1, W, Dc), BF16),
                pltpu.VMEM((NM, W, Dc), F32),
                pltpu.VMEM((FM, W, Dc), BF16),
                pltpu.VMEM((O, W, Dc), BF16),
                dma((X,)), dma((X,)), dma((2,)), dma((2,)), dma((X, 2)), dma((X, 2)), dma(()),
                dma((NM, 3, J)), dma((NM, 3, J)), dma((NM, 3)),
                dma((NM, 3, J)), dma((NM, 3, J)), dma((NM, 3)),
                dma((O,)), dma((FM,)), dma((O,)),
                dma((NM, H)), dma((NM, H)), dma((NM, H)), dma((NM, H)),
                dma((NM,)), dma((NM,)), dma((NM, H)), dma((NM, H)),
                dma((FM,)), dma((O,)),
            ],
            compiler_params=pltpu.CompilerParams(
                collective_id=0, has_side_effects=True, vmem_limit_bytes=56 * 1024 * 1024
            ),
        )(bucket_of, lengths, counts, queries, keys, values, out_grad, w_out)
        vmem = pl.BlockSpec(memory_space=pltpu.VMEM)
        return pl.pallas_call(
            store,
            out_shape=(grad, grad, grad, jax.ShapeDtypeStruct((R, Dc), F32)),
            in_specs=[vmem] * 4,
            out_specs=(hbm,) * 4,
            scratch_shapes=[dma((4, PARTS))],
            compiler_params=pltpu.CompilerParams(vmem_limit_bytes=1024 * 1024),
        )(*held)

    rows = P(("grp", "sp"), None)
    return jax.shard_map(
        shards,
        mesh=mesh,
        in_specs=(P(), P(), P(), rows, rows, rows, rows, P("sp", "grp")),
        out_specs=(rows, rows, rows, P("sp", "grp")),
        check_vma=False,
    )
```

```python
import functools

import jax
import jax.numpy as jnp
from jax import lax
from jax.experimental import pallas as pl
from jax.experimental.pallas import tpu as pltpu
from jax.sharding import PartitionSpec as P

HEAD_DIM = 128
SEQS = 2
LAG = 2
PARTS = 2
MESH = pl.DeviceIdType.MESH
F32 = jnp.float32
BF16 = jnp.bfloat16


def dot(a, b, ca, cb):
    return lax.dot_general(a, b, (((ca,), (cb,)), ((), ())), preferred_element_type=F32)


END_ORDER = (
    ("x3", 0), ("ogz", 0), ("ogz", 1), ("w0", 0), ("w0", 1), ("ogx", 0), ("x1", 0), ("x3", 1),
    ("x1", 1), ("wy", 0), ("x3", 2), ("x1", 2), ("x2", 1), ("relay", 0), ("x3", 3), ("x2", 0),
    ("ogr", 1), ("x1", 3), ("x3", 4), ("fwd", 0), ("ogr", 0), ("x2", 2), ("x1", 4),
)
MIDDLE_ORDER = (
    ("wy", 0), ("x3", 1), ("x3", 2), ("ogz", 1), ("x1", 0), ("x3", 0), ("w0", 1), ("w0", 0),
    ("x2", 0), ("ogx", 0), ("ogr", 0), ("ogr", 1), ("relay", 0), ("x2", 1), ("fwd", 0), ("x2", 2),
    ("relay", 1), ("ogz", 0), ("x2", 3), ("x2", 4), ("x1", 2), ("x1", 1), ("relay", 2),
)


def schedule(role, O, E, NM):
    if (O, E) == (2, 1):
        return MIDDLE_ORDER if role == 1 else END_ORDER
    w0 = [("w0", m) for m in range(O)]
    start = [("ogz", 0), ("ogz", 1), ("ogx", 0), ("wy", 0)]
    og_relays = [("ogr", 0), ("ogr", 1)]
    chunks = [(kind, ch) for ch in range(1, NM) for kind in ("x1", "x3", "x2")]
    w_relays = [("relay", 0), ("fwd", 0)] + [("relay", n) for n in range(1, NM - O)]
    first = [("x1", 0), ("x3", 0), ("x2", 0)] + og_relays + chunks + w_relays
    return start + w0 + first if role == 0 else w0[E:] + w0[:E] + start + first


def kernel(
    G, S, D, W, E,
    bucket_ref, length_ref, count_ref, q_ref, k_ref, v_ref, og_ref, w_ref,
    gq_ref, gk_ref, gv_ref, gw_ref,
    qh, kh, vh, dqs, dks, dvs, og, w, d_attn, attn_t, gs1, gr1, gown, gs2, gr2, gkeep, gs3, gr3,
    og_s, og_r, oz_s, oz_r, or_s, or_r, og_l, x_s, x_r, x_l, b_s, b_r, b_l,
    w0_s, w0_r, w_l, wy_s, wy_r, ws_s, ws_r, g1_s, g1_r, g2_s, g2_r, g3_s, g3_r,
):
    J = S // SEQS
    X = J // 2
    H = G // 2
    T = q_ref.shape[0]
    HD = q_ref.shape[1]
    L = J * T
    O = HD // S // W
    FM = 2 * O - E
    NM = FM + O
    NEAR = O - E
    BIG = 4 * O
    Dc = D // G
    scale = HEAD_DIM ** (-0.5)

    g = lax.axis_index("grp")
    s = lax.axis_index("sp")
    z, jx = s // X, s % X
    u, jz = z // 2, z % 2
    mid = (u + jz) % 2
    j = jz * X + jx
    h, c = g // 2, g % 2
    sibling = (h * 2 + 1 - c, s)

    def at(uu, mm, x):
        return (uu * 2 + (uu + mm) % 2) * X + x

    def foreign_of(mm):
        return E + mm * (FM - E)

    foreign = foreign_of(mid)
    mine = foreign + O
    theirs = foreign_of(1 - mid) + O

    def foreign_source(n, mm):
        far = mm * ((n + BIG - NEAR) // BIG)
        return 1 - far, n + mm * ((1 - far) * E - far * NEAR)

    def to_h(e):
        return ((h + e) % H * 2 + c, s)

    def seq_x(d):
        return (jx + d % X) % X

    def seq_from_x(d):
        return (jx - d % X + X) % X

    def seq_mid(d):
        return (mid + d // X) % 2

    def seq_row(d, x):
        return (jz + d // X) % 2 * X + x

    def seq_peer(d):
        return (g, at(u, seq_mid(d), seq_x(d)))

    across_mid = (g, at(1 - u, 1, jx))
    across_edge = (g, at(1 - u, 0, jx))

    peers = [seq_peer(d) for d in range(1, J)] + [to_h(e) for e in range(1, H)] + [sibling, across_mid]
    barrier = pltpu.get_barrier_semaphore()
    for peer in peers:
        pl.semaphore_signal(barrier, inc=1, device_id=peer, device_id_type=MESH)

    @pl.when(mid == 1)
    def _():
        pl.semaphore_signal(barrier, inc=1, device_id=across_edge, device_id_type=MESH)

    def remote(src, dst, ss, rs, dev):
        return pltpu.make_async_remote_copy(
            src_ref=src, dst_ref=dst, send_sem=ss, recv_sem=rs, device_id=dev, device_id_type=MESH
        )

    def col_of(ch, mm, x):
        first = foreign_of(mm)
        own = (ch + BIG - first) // BIG
        source_mid, piece_at = foreign_source(ch, mm)
        source = own * at(u, mm, x) + (1 - own) * at(1 - u, source_mid, x)
        return pl.multiple_of((source * O + own * (ch - first) + (1 - own) * piece_at) * W, W)

    def rows(jj):
        return pl.ds(pl.multiple_of(jj * T, T), T)

    xs = ((q_ref, qh), (k_ref, kh), (v_ref, vh))
    bs = ((dqs, gq_ref), (dks, gk_ref), (dvs, gv_ref))

    def w_rows(m):
        return w_ref.at[pl.ds(m * W, W)]

    def w0_copy(m):
        target_mid, n = (1 - mid, m) if m < E else (1, m - E)
        n = (1 - mid) * (NEAR + m) + mid * n
        return remote(w_rows(m), w.at[n, g], w0_s.at[m], w0_r.at[n], (g, at(1 - u, target_mid, jx)))

    def w0_arrival(n):
        return remote(w.at[n, g], w.at[n, g], w0_s.at[0], w0_r.at[n], across_mid)

    def wy_copy(src, ch, e):
        return remote(src, w.at[ch, g], wy_s.at[ch, e], wy_r.at[ch, e], to_h(e))

    def ws_own(src, ch):
        return remote(src, w.at[ch, g], ws_s.at[ch, 0], ws_r.at[ch, 0], sibling)

    def ws_copy(ch, e):
        src = (h - e + H) % H * 2 + c
        return remote(w.at[ch, src], w.at[ch, src], ws_s.at[ch, e], ws_r.at[ch, e], sibling)

    def wy_arrival(ch, e):
        src = (h - e + H) % H * 2 + c
        return remote(w.at[ch, src], w.at[ch, src], wy_s.at[ch, e], wy_r.at[ch, e], to_h(e))

    def ws_arrival(ch, e):
        src = (h - e + H) % H * 2 + 1 - c
        return remote(w.at[ch, src], w.at[ch, src], ws_s.at[ch, e], ws_r.at[ch, e], sibling)

    mate = (1 - jz) * X + jx

    def og_x_peer(e):
        return (g, u * J + jz * X + (jx + e) % X)

    def piece(jj, p):
        return og.at[pl.ds(pl.multiple_of(jj * T + p * (T // 2), T // 2), T // 2)]

    def og_z(p):
        src = og_ref.at[pl.ds(p * (T // 2), T // 2)]
        return remote(src, piece(j, p), oz_s.at[p], oz_r.at[p], (g, u * J + mate))

    def og_z_arrival(p):
        src = og_ref.at[pl.ds(p * (T // 2), T // 2)]
        return remote(src, piece(mate, p), oz_s.at[p], oz_r.at[p], (g, u * J + mate))

    def og_x(e):
        return remote(og_ref, og.at[rows(j)], og_s.at[e], og_r.at[e], og_x_peer(e))

    def og_x_arrival(e):
        src = rows(jz * X + (jx - e + X) % X)
        return remote(og_ref, og.at[src], og_s.at[e], og_r.at[e], og_x_peer(e))

    def og_relay(e, p):
        block = piece(mate, p)
        return remote(block, block, or_s.at[e, p], or_r.at[e, p], og_x_peer(e))

    def og_relay_arrival(e, p):
        block = piece((1 - jz) * X + (jx - e + X) % X, p)
        return remote(block, block, or_s.at[e, p], or_r.at[e, p], og_x_peer(e))

    def x_copy(ch, i, d):
        src, dst = xs[i]
        cols = pl.ds(col_of(ch, seq_mid(d), seq_x(d)), W)
        return remote(
            src.at[:, cols], dst.at[ch, rows(j)], x_s.at[ch, i, d], x_r.at[ch, i, d], seq_peer(d)
        )

    def x_arrival(ch, i, d):
        src, dst = xs[i]
        return remote(
            src.at[:, pl.ds(0, W)], dst.at[ch, rows(seq_row(d, seq_from_x(d)))],
            x_s.at[ch, i, d], x_r.at[ch, i, d], seq_peer(d),
        )

    def x_local(ch, i):
        src, dst = xs[i]
        return pltpu.make_async_copy(
            src.at[:, pl.ds(col_of(ch, mid, jx), W)], dst.at[ch, rows(j)], x_l.at[ch, i]
        )

    def b_copy(ch, i, d):
        src, dst = bs[i]
        return remote(
            src.at[ch, rows(seq_row(d, seq_x(d)))], dst.at[:, pl.ds(col_of(ch, mid, jx), W)],
            b_s.at[ch, i, d], b_r.at[ch, i, d], seq_peer(d),
        )

    def b_arrival(ch, i, d):
        src, dst = bs[i]
        return remote(
            src.at[ch, rows(j)], dst.at[:, pl.ds(col_of(ch, seq_mid(d), seq_from_x(d)), W)],
            b_s.at[ch, i, d], b_r.at[ch, i, d], seq_peer(d),
        )

    def b_local(ch, i):
        src, dst = bs[i]
        return pltpu.make_async_copy(
            src.at[ch, rows(j)], dst.at[:, pl.ds(col_of(ch, mid, jx), W)], b_l.at[ch, i]
        )

    og_own = pltpu.make_async_copy(og_ref, og.at[rows(j)], og_l)

    def w_local(m):
        return pltpu.make_async_copy(w_rows(m), w.at[foreign + m, g], w_l.at[m])

    def g1_copy(ch):
        return remote(gs1.at[ch], gr1.at[ch], g1_s.at[ch], g1_r.at[ch], sibling)

    def g2_copy(ch, e):
        return remote(gs2.at[ch, e - 1], gr2.at[ch, e - 1], g2_s.at[ch, e], g2_r.at[ch, e], to_h(e))

    def g3_copy(n):
        source_mid, m = foreign_source(n, mid)
        return remote(
            gs3.at[n], gr3.at[m], g3_s.at[n], g3_r.at[m], (g, at(1 - u, source_mid, jx))
        )

    def g3_arrival(m):
        return remote(gr3.at[m], gr3.at[m], g3_s.at[0], g3_r.at[m], across_mid)

    og_own.start()
    for m in range(O):
        w_local(m).start()

    def local_chunk(ch, carry):
        for i in range(3):
            x_local(ch, i).start()
        return carry

    lax.fori_loop(0, mine, local_chunk, 0)
    pl.semaphore_wait(barrier, len(peers) + mid)

    def relay_w0(n):
        w0_arrival(n).wait_recv()
        for e in range(1, H):
            wy_copy(w.at[n, g], n, e).start()
        ws_own(w.at[n, g], n).start()

    def forward_w(ch):
        for e in range(1, H):
            wy_arrival(ch, e).wait_recv()
            ws_copy(ch, e).start()

    def issue(kind, n, role):
        theirs_n = E + (1 - role) * (FM - E) + O
        mine_n = E + role * (FM - E) + O
        first = mine_n - O
        if kind == "w0" and n < O:
            w0_copy(n).start()
        elif kind == "ogz":
            og_z(n).start()
        elif kind == "ogx":
            for e in range(1, X):
                og_x(e).start()
        elif kind == "ogr":
            og_z_arrival(n).wait_recv()
            for e in range(1, X):
                og_relay(e, n).start()
        elif kind == "wy":
            for m in range(O):
                for e in range(1, H):
                    wy_copy(w_rows(m), first + m, e).start()
                ws_own(w_rows(m), first + m).start()
        elif kind == "x1" and n < theirs_n:
            for i in range(3):
                x_copy(n, i, X).start()
        elif kind == "x3" and n < theirs_n:
            for i in range(3):
                for d in range(X + 1, J):
                    x_copy(n, i, d).start()
        elif kind == "x2" and n < mine_n:
            for i in range(3):
                for d in range(1, X):
                    x_copy(n, i, d).start()
        elif kind == "relay" and n < first:
            relay_w0(n)
        elif kind == "fwd":
            forward_w(n)

    for role in range(2):
        @pl.when(mid == role)
        def _():
            for kind, n in schedule(role, O, E, NM):
                issue(kind, n, role)

    for m in range(O):
        w_local(m).wait()
    og_own.wait()
    for e in range(1, X):
        og_x_arrival(e).wait_recv()
        og_relay_arrival(e, 0).wait_recv()
        og_relay_arrival(e, 1).wait_recv()

    seq_len = length_ref[bucket_ref[g]]
    total = count_ref[bucket_ref[0]]
    for other in range(1, G):
        total = total + count_ref[bucket_ref[other]]
    weight = jnp.full((1, 1), count_ref[bucket_ref[g]], jnp.int32).astype(F32) / jnp.full(
        (1, 1), total, jnp.int32
    ).astype(F32)
    keep_key = lax.broadcasted_iota(jnp.int32, (L, 1), 0) < seq_len
    keep_col = lax.broadcasted_iota(jnp.int32, (1, L), 1) < seq_len

    def compute(ch):
        for i in range(3):
            x_local(ch, i).wait()
            for d in range(1, J):
                x_arrival(ch, i, d).wait_recv()
        for e in range(H):
            ws_arrival(ch, e).wait_recv()
        acc = dot(og[:, 0:Dc], w[ch, 0], 1, 1)
        for gg in range(1, G):
            acc = acc + dot(og[:, gg * Dc:(gg + 1) * Dc], w[ch, gg], 1, 1)
        d_attn[...] = jnp.where(keep_key, acc, 0.0).astype(BF16)

        @pl.when(ch >= 1)
        def _():
            across_groups(ch - 1)

        for n in range(W // HEAD_DIM):
            lanes = slice(n * HEAD_DIM, (n + 1) * HEAD_DIM)
            q = qh[ch, :, lanes]
            k = kh[ch, :, lanes]
            v = vh[ch, :, lanes]
            do = d_attn[:, lanes]
            scores = jnp.where(keep_key, dot(k, q, 1, 1) * scale, -1e30)
            top = jnp.max(scores, axis=0, keepdims=True)
            ex = jnp.exp(scores - top)
            probs = ex * (1.0 / jnp.sum(ex, axis=0, keepdims=True))
            low = probs.astype(BF16)
            attn = dot(v, low, 0, 0)
            attn_t[lanes, :] = jnp.where(keep_col, attn, 0.0).astype(BF16)
            dp = dot(v, do, 1, 1)
            delta = jnp.sum(probs * dp, axis=0, keepdims=True)
            ds = (probs * (dp - delta)).astype(BF16)
            dvs[ch, :, lanes] = dot(low, do, 1, 0).astype(BF16)
            dks[ch, :, lanes] = (dot(ds, q, 1, 0) * scale).astype(BF16)
            dqs[ch, :, lanes] = (dot(k, ds, 0, 0) * scale).T.astype(BF16)

        def send_back(ds):
            for d in ds:
                for i in range(3):
                    b_copy(ch, i, d).start()

        @pl.when(mid == 0)
        def _():
            send_back(range(1, J))

        @pl.when(mid == 1)
        def _():
            send_back(list(range(X + 1, J)) + list(range(1, X)) + [X])

        for i in range(3):
            b_local(ch, i).start()

        @pl.when(ch + 1 < mine)
        def _():
            forward_w(ch + 1)

        @pl.when(ch >= LAG)
        def _():
            across_halves(ch - LAG)

        for hh in range(H):
            low_c, high_c = (
                dot(attn_t[...], og[:, gg * Dc:(gg + 1) * Dc], 1, 0) * weight
                for gg in (2 * hh, 2 * hh + 1)
            )
            gown[ch, hh] = jnp.where(c == 0, low_c, high_c)
            gs1[ch, hh] = jnp.where(c == 0, high_c, low_c).astype(BF16)
        g1_copy(ch).start()

    def across_groups(ch):
        g1_copy(ch).wait_recv()
        for e in range(1, H):
            to = (h + e) % H
            gs2[ch, e - 1] = (gown[ch, to] + gr1[ch, to].astype(F32)).astype(BF16)
            g2_copy(ch, e).start()
        gkeep[ch] = gown[ch, h] + gr1[ch, h].astype(F32)

    def across_halves(ch):
        part = gkeep[ch]
        for e in range(1, H):
            g2_copy(ch, e).wait_recv()
            part = part + gr2[ch, e - 1].astype(F32)

        @pl.when(ch < foreign)
        def _():
            gs3[ch] = part.astype(BF16)
            g3_copy(ch).start()

        @pl.when(ch >= foreign)
        def _():
            gkeep[ch] = part

    def step(n, carry):
        compute(n)
        return carry

    lax.fori_loop(0, mine, step, 0)
    across_groups(mine - 1)
    for n in range(LAG, 0, -1):
        @pl.when(mine >= n)
        def _():
            across_halves(mine - n)

    for m in range(O):
        g3_arrival(m).wait_recv()
        gw_ref[m * W:(m + 1) * W, :] = gkeep[foreign + m] + gr3[m].astype(F32)

    og_z(0).wait_send()
    og_z(1).wait_send()
    for e in range(1, X):
        og_x(e).wait_send()
        og_relay(e, 0).wait_send()
        og_relay(e, 1).wait_send()
    for m in range(O):
        w0_copy(m).wait_send()

    def drain(ch, carry):
        @pl.when(ch < foreign)
        def _():
            g3_copy(ch).wait_send()

        @pl.when(ch < mine)
        def _():
            ws_own(w.at[ch, g], ch).wait_send()
            for e in range(1, H):
                ws_copy(ch, e).wait_send()
                wy_copy(w.at[ch, g], ch, e).wait_send()
                g2_copy(ch, e).wait_send()
            g1_copy(ch).wait_send()
            for i in range(3):
                b_local(ch, i).wait()
                for d in range(1, J):
                    b_copy(ch, i, d).wait_send()
                for d in range(1, X):
                    x_copy(ch, i, d).wait_send()
                    b_arrival(ch, i, d).wait_recv()

        @pl.when(ch < theirs)
        def _():
            for i in range(3):
                for d in range(X, J):
                    x_copy(ch, i, d).wait_send()
                    b_arrival(ch, i, d).wait_recv()

        return carry

    lax.fori_loop(0, NM, drain, 0)


def store(*refs):
    sems = refs[-1]
    copies = []
    for i in range(4):
        rows = refs[i].shape[0] // PARTS
        for n in range(PARTS):
            part = pl.ds(n * rows, rows)
            copies.append(pltpu.make_async_copy(refs[i].at[part], refs[4 + i].at[part], sems.at[i, n]))
    for copy in copies:
        copy.start()
    for copy in copies:
        copy.wait()


def solution(mesh):
    G, S = mesh.shape["grp"], mesh.shape["sp"]
    J, H = S // SEQS, G // 2
    X = J // 2

    def shards(bucket_of, lengths, counts, queries, keys, values, out_grad, w_out):
        T, HD = queries.shape
        D = out_grad.shape[1]
        L, R, Dc = J * T, HD // S, D // G
        W = 256 if R % 256 == 0 else 128
        O = R // W
        E = O // 2
        NM = 3 * O - E
        FM = NM - O
        dma = pltpu.SemaphoreType.DMA
        head = pltpu.VMEM((NM, L, W), BF16)
        smem = pl.BlockSpec(memory_space=pltpu.SMEM)
        hbm = pl.BlockSpec(memory_space=pltpu.HBM)
        grad = jax.ShapeDtypeStruct((T, HD), BF16)
        held = pl.pallas_call(
            functools.partial(kernel, G, S, D, W, E),
            out_shape=(pltpu.VMEM((T, HD), BF16),) * 3 + (pltpu.VMEM((R, Dc), F32),),
            in_specs=[smem] * 3 + [hbm] * 5,
            out_specs=(pl.BlockSpec(memory_space=pltpu.VMEM),) * 4,
            scratch_shapes=[head] * 6 + [
                pltpu.VMEM((L, D), BF16),
                pltpu.VMEM((NM, G, W, Dc), BF16),
                pltpu.VMEM((L, W), BF16),
                pltpu.VMEM((W, L), BF16),
                pltpu.VMEM((NM, H, W, Dc), BF16),
                pltpu.VMEM((NM, H, W, Dc), BF16),
                pltpu.VMEM((NM, H, W, Dc), F32),
                pltpu.VMEM((NM, H - 1, W, Dc), BF16),
                pltpu.VMEM((NM, H - 1, W, Dc), BF16),
                pltpu.VMEM((NM, W, Dc), F32),
                pltpu.VMEM((FM, W, Dc), BF16),
                pltpu.VMEM((O, W, Dc), BF16),
                dma((X,)), dma((X,)), dma((2,)), dma((2,)), dma((X, 2)), dma((X, 2)), dma(()),
                dma((NM, 3, J)), dma((NM, 3, J)), dma((NM, 3)),
                dma((NM, 3, J)), dma((NM, 3, J)), dma((NM, 3)),
                dma((O,)), dma((FM,)), dma((O,)),
                dma((NM, H)), dma((NM, H)), dma((NM, H)), dma((NM, H)),
                dma((NM,)), dma((NM,)), dma((NM, H)), dma((NM, H)),
                dma((FM,)), dma((O,)),
            ],
            compiler_params=pltpu.CompilerParams(
                collective_id=0, has_side_effects=True, vmem_limit_bytes=56 * 1024 * 1024
            ),
        )(bucket_of, lengths, counts, queries, keys, values, out_grad, w_out)
        vmem = pl.BlockSpec(memory_space=pltpu.VMEM)
        return pl.pallas_call(
            store,
            out_shape=(grad, grad, grad, jax.ShapeDtypeStruct((R, Dc), F32)),
            in_specs=[vmem] * 4,
            out_specs=(hbm,) * 4,
            scratch_shapes=[dma((4, PARTS))],
            compiler_params=pltpu.CompilerParams(vmem_limit_bytes=1024 * 1024),
        )(*held)

    rows = P(("grp", "sp"), None)
    return jax.shard_map(
        shards,
        mesh=mesh,
        in_specs=(P(), P(), P(), rows, rows, rows, rows, P("sp", "grp")),
        out_specs=(rows, rows, rows, P("sp", "grp")),
        check_vma=False,
    )
```
